32 devices in a mesh: lon: 4 (over y, x), lat: 4 (over z), mem: 2 (over core).
Axes of the slice: x: 2, y: 2, z: 4, core: 2. Of those that a mesh axis runs over, the one named last changes fastest.
Arguments:
- north_vel: bfloat16 [2, 4, 75, 128, 512], P('mem', None, None, 'lat', 'lon'), may hold values from -6 to 6
- up_vel: bfloat16 [2, 4, 75, 128, 512], P('mem', None, None, 'lat', 'lon'), may hold values from -6 to 6
- dens_class: int32 [2, 4, 75, 128, 512], P('mem', None, None, 'lat', 'lon'), may hold values from 0 to 79
- thickness: int32 [75, 128, 512], P(None, 'lat', 'lon'), may hold values from 0 to 2000
- basin_id: int32 [128, 512], P('lat', 'lon'), may hold values from 0 to 3
Outputs:
- depth_mean: float32 [4, 4, 2, 75, 128], P('lon', None, None, None, 'lat')
- depth_spread: float32 [4, 4, 2, 75, 128], P('lon', None, None, None, 'lat')
- class_mean: float32 [4, 4, 2, 80, 128], P('lon', None, None, None, 'lat')
- class_spread: float32 [4, 4, 2, 80, 128], P('lon', None, None, None, 'lat')
The draws below stay inside these ranges and needn't reach their ends.
Inputs may be any that keep to these rules, and one draw needn't show every extreme that they name: `basin_id`: 0 marks land; 1 to 3 name the basins. `thickness`: thousandths of a unit layer; 0 marks a cell below the sea floor.
All inputs are finite; a program needn't handle non-finite values.
Results may differ from the reference program's by a relative error of at most 0.0029.
Values sent between devices are 32-bit elements; how exact they have to be, the bound alone decides.
No kernel may reach another device: no remote copies, remote signals or barrier semaphores. Data moves between devices by JAX's collectives and lax.ppermute only.
A program may use at most 128 MiB of HBM per device.

```python
import math
import jax
import jax.numpy as jnp
from jax import lax

MONTHS = 4
LEVELS = 75
CLASSES = 80
BASINS = 3
NLON = 512
NLAT = 128
MEMBERS = 2


def place_ends(array, rng, least, top_value):
    extent = array.shape
    index_at = [jax.random.randint(jax.random.fold_in(rng, axis), (), 0, extent[axis]) for axis in range(len(extent))]
    array = array.at[tuple(index_at)].set(least)
    longest = extent.index(max(extent))
    index_at[longest] = (index_at[longest] + 1) % extent[longest]
    return array.at[tuple(index_at)].set(top_value)


def level_of(own_key, extent, shards, low, top_value):
    factor_of, own = 1.0, jax.random.fold_in(own_key, 6)
    for position, shards_of in shards:
        heights = jnp.exp(jax.random.uniform(jax.random.fold_in(own, position), (shards_of,), jnp.float32, low / len(shards), top_value / len(shards)))
        factor_of = factor_of * jnp.repeat(heights, extent[position] // shards_of).reshape([-1 if axis == position else 1 for axis in range(len(extent))])
    return factor_of


def scatter_about(own_key, shape, width, most, pieces=(), held_as=jnp.bfloat16):
    entries = width * jax.random.normal(own_key, shape, jnp.float32)
    if pieces:
        entries = entries * level_of(own_key, shape, pieces, -0.22, 0.18)
    return jnp.clip(entries, -most, most).astype(held_as)


def setup_inputs(seed: int = 0) -> dict:
    arg_keys = jax.random.split(jax.random.key(seed), 6)
    north_vel = scatter_about(arg_keys[0], (MEMBERS, MONTHS, LEVELS, NLAT, NLON), 1.0, 6.0, ((0, 2), (3, 4), (4, 4)))
    up_vel = scatter_about(arg_keys[1], (MEMBERS, MONTHS, LEVELS, NLAT, NLON), 1.0, 6.0, ((0, 2), (3, 4), (4, 4)))
    dens_class = place_ends(jax.random.randint(arg_keys[2], (MEMBERS, MONTHS, LEVELS, NLAT, NLON), 0, CLASSES), jax.random.fold_in(arg_keys[2], 1), 0, CLASSES - 1).astype(jnp.int32)
    thickness = place_ends(jax.random.randint(arg_keys[3], (LEVELS, NLAT, NLON), 0, 2001), jax.random.fold_in(arg_keys[3], 1), 0, 2000).astype(jnp.int32)
    basin_id = place_ends(jax.random.randint(arg_keys[4], (NLAT, NLON), 0, BASINS + 1), jax.random.fold_in(arg_keys[4], 1), 0, BASINS).astype(jnp.int32)
    return {"north_vel": north_vel, "up_vel": up_vel, "dens_class": dens_class, "thickness": thickness, "basin_id": basin_id}


north_unit = 0.02
up_unit = 0.01

def class_sums(north_flux, rise_flux, dens_class, basin_masks):
    months, levels, lat_rows, lon_cells = north_flux.shape
    weighted = jnp.stack([north_flux, rise_flux], 2).reshape(months * levels, 2, lat_rows, lon_cells)
    classes_flat = dens_class.reshape(months * levels, lat_rows, lon_cells)
    class_ids = jnp.arange(CLASSES, dtype=jnp.int32)

    def one_level(packed):
        onehot = (packed[1][..., None] == class_ids).astype(jnp.float32)
        return jnp.einsum('sji,bji,jic->bscj', packed[0], basin_masks, onehot, precision=lax.Precision.HIGHEST)
    per_level = lax.map(one_level, (weighted, classes_flat))
    return lax.optimization_barrier(jnp.sum(per_level.reshape(months, levels, BASINS, 2, CLASSES, lat_rows), axis=1))

def member_tables(north_vel, up_vel, dens_class, thickness, basin_id, first_row, lat_total):
    months, levels, lat_rows, lon_cells = north_vel.shape
    row_index = first_row + jnp.arange(lat_rows, dtype=jnp.int32)
    latitude = (-78.0 + 156.0 * (row_index.astype(jnp.float32) + 0.5) / lat_total) * (math.pi / 180.0)
    zonal_width = jnp.cos(latitude)
    layer_depth = thickness.astype(jnp.float32) * 0.001
    wet_cells = (thickness > 0).astype(jnp.float32)
    north_flux = north_vel.astype(jnp.float32) * (north_unit * zonal_width)[None, None, :, None] * layer_depth[None]
    rise_flux = up_vel.astype(jnp.float32) * (up_unit * zonal_width)[None, None, :, None] * wet_cells[None]
    north_flux = north_flux.astype(jnp.bfloat16).astype(jnp.float32)
    rise_flux = rise_flux.astype(jnp.bfloat16).astype(jnp.float32)
    basin_masks = (basin_id[None] == jnp.arange(1, BASINS + 1, dtype=jnp.int32)[:, None, None]).astype(jnp.float32)
    north_depth = jnp.einsum('mkji,bji->mbkj', north_flux, basin_masks, precision=lax.Precision.HIGHEST)
    rise_depth = jnp.einsum('mkji,bji->mbkj', rise_flux, basin_masks, precision=lax.Precision.HIGHEST)
    depth_tab = jnp.stack([north_depth, rise_depth], 2)
    class_tab = class_sums(north_flux, rise_flux, dens_class, basin_masks)
    return (class_tab, depth_tab)

def with_global(tables):
    return jnp.concatenate([lax.optimization_barrier(jnp.sum(tables, axis=2, keepdims=True)), tables], 2)

def moments(stack_moc):
    members = stack_moc.shape[0]
    mean_val = lax.optimization_barrier(jnp.sum(stack_moc, 0)) / members
    spread_val = jnp.sqrt(lax.optimization_barrier(jnp.sum(jnp.square(stack_moc - mean_val), 0)) / (members - 1))
    return (mean_val, spread_val)

def reference(north_vel, up_vel, dens_class, thickness, basin_id):

    def one_member(packed):
        return member_tables(packed[0], packed[1], packed[2], thickness, basin_id, 0, NLAT)
    class_tab, depth_tab = lax.map(one_member, (north_vel, up_vel, dens_class))
    class_reg = with_global(class_tab)
    depth_reg = with_global(depth_tab)
    class_moc = jnp.stack([jnp.cumsum(class_reg[:, :, :, 0], axis=3), jnp.cumsum(jnp.cumsum(class_reg[:, :, :, 1], axis=4), axis=3)], 3)
    depth_moc = jnp.stack([jnp.cumsum(depth_reg[:, :, :, 0], axis=3), jnp.cumsum(depth_reg[:, :, :, 1], axis=4)], 3)
    depth_mean, depth_spread = moments(depth_moc)
    class_mean, class_spread = moments(class_moc)
    return (depth_mean, depth_spread, class_mean, class_spread)
```

```python
import math

import jax
import jax.numpy as jnp
from jax import lax
from jax.experimental import pallas as pl
from jax.experimental.pallas import tpu as pltpu
from jax.sharding import PartitionSpec as P

CLASSES = 80
BASINS = 3
LOW = 8
HIGHS = CLASSES // LOW
SUB = 8
SLOTS = 256 // SUB
GROUPS = 2

north_unit = 0.02
up_unit = 0.01

F8 = jnp.float8_e4m3fn
BF = jnp.bfloat16
F32 = jnp.float32


def tables_kernel(levels, pairs, cut, mon, n_ref, u_ref, d_ref, t_ref, b_ref, w_ref, hc_ref, oc_ref, od_ref, f_s):
    def body(*accs):
        ca, da, db = accs[0:2], accs[2:4], accs[4:6]
        row = lax.broadcasted_iota(jnp.int32, (SUB, 256), 0)
        lane = lax.broadcasted_iota(jnp.int32, (SUB, 256), 1)
        diag = row == (lane & (SUB - 1))
        digits = hc_ref[...]
        offs, cn, cu = [], [], []
        for q in range(GROUPS):
            rows = slice(q * SUB, (q + 1) * SUB)
            b = b_ref[rows, :]
            offs.append(jnp.where(b > 0, (b - 1) * HIGHS, 2 * SLOTS))
            cn.append(w_ref[rows, :] * north_unit)
            cu.append(w_ref[rows, :] * up_unit)
        for p in range(pairs):
            lhs = [[] for _ in range(GROUPS)]
            rhs = [[] for _ in range(GROUPS)]
            for e in range(2):
                k = p + e * pairs
                lanes = slice(e * 128, (e + 1) * 128)
                if k >= levels:
                    for q in range(GROUPS):
                        lhs[q].append(jnp.zeros((128, 128), BF))
                        rhs[q].append(jnp.zeros((256, 128), F8))
                        f_s[q, p * 16 : (p + 1) * 16, lanes] = jnp.zeros((16, 128), BF)
                    continue
                n16 = n_ref[0, k].astype(F32)
                u16 = u_ref[0, k].astype(F32)
                for q in range(GROUPS):
                    rows = slice(q * SUB, (q + 1) * SUB)
                    t = t_ref[k, rows, :]
                    north = n16[rows] * cn[q] * (t.astype(F32) * 0.001)
                    rise = jnp.where(t > 0, u16[rows] * cu[q], 0.0)
                    flux = jnp.concatenate([north, rise], 0).astype(BF)
                    f_s[q, p * 16 : (p + 1) * 16, lanes] = flux
                    d = d_ref[0, k, rows, :]
                    high = ((d >> 3) + offs[q]).astype(F32)
                    low = (d & (LOW - 1)).astype(F32)
                    high = jnp.concatenate([high, high], 0).astype(BF)
                    low = jnp.concatenate([low, low], 0).astype(BF)
                    lhs[q].append(
                        jnp.concatenate([jnp.where(low == BF(x), flux, BF(0)) for x in range(LOW)], 0)
                    )
                    hit = jnp.concatenate([high] * 16, 0) == digits
                    rhs[q].append(jnp.where(hit, F8(1), F8(0)))
            for q in range(GROUPS):
                pltpu.matmul_push_rhs(
                    jnp.concatenate(rhs[q], 1), staging_register=p % 2, mxu_index=q, transpose=True
                )
            for q in range(GROUPS):
                pltpu.matmul_acc_lhs(ca[q], jnp.concatenate(lhs[q], 1), load_staged_rhs=p % 2)
        for q in range(GROUPS):
            b = b_ref[q * SUB : (q + 1) * SUB, :]
            mask = jnp.concatenate(
                [jnp.where(b == i + 1, 1.0, 0.0) for i in range(BASINS)] + [jnp.zeros((SUB, 128), F32)], 0
            )
            zero = jnp.zeros((32, 128), F32)
            held = jnp.concatenate(
                [
                    jnp.concatenate([mask, zero], 1),
                    jnp.concatenate([zero, mask], 1),
                    jnp.zeros((192, 256), F32),
                ],
                0,
            )
            pltpu.matmul_push_rhs(held.astype(F8), staging_register=pairs % 2, mxu_index=q, transpose=True)
        for q in range(GROUPS):
            pltpu.matmul_acc_lhs(da[q], f_s[q, 0 : cut * 16, :], load_staged_rhs=pairs % 2)
            pltpu.matmul_acc_lhs(db[q], f_s[q, cut * 16 : pairs * 16, :])
        for q in range(GROUPS):
            x = pltpu.matmul_pop(ca[q]).reshape(LOW, 2, SUB, 256)
            x = jnp.sum(jnp.where(diag[None, None], x, 0.0), axis=2)
            oc_ref[0, q, 0] = x[:, 0]
            oc_ref[0, q, 1] = x[:, 1]
        for q in range(GROUPS):
            for a, first, last in ((da[q], 0, cut), (db[q], cut, pairs)):
                x = pltpu.matmul_pop(a)[:, :128].reshape(last - first, 2, SUB, 128)
                x = jnp.sum(jnp.where(diag[None, None, :, :128], x, 0.0), axis=2)
                od_ref[0, q, 0, first:last, :] = x[:, 0]
                od_ref[0, q, 1, first:last, :] = x[:, 1]

    def acc(q, rows):
        return pltpu.ACC(q)((rows, 256), F32)

    pl.run_scoped(
        body, acc(0, 128), acc(1, 128), acc(0, cut * 16), acc(1, cut * 16),
        acc(0, (pairs - cut) * 16), acc(1, (pairs - cut) * 16),
    )


def lon_tables(order, north_vel, up_vel, dens_class, thickness, basin_id, width):
    _, levels, lat_rows, lon_cells = north_vel.shape
    pairs = (levels + 1) // 2
    cut = 24 if pairs > 24 else pairs // 2
    tall = GROUPS * SUB
    blocks = lat_rows // SUB
    digits = jnp.broadcast_to((jnp.arange(256, dtype=jnp.int32) // SUB).astype(BF)[:, None], (256, 128))
    padded = -(-pairs // 8) * 8

    def month_block():
        return pl.BlockSpec((1, levels, tall, lon_cells), lambda m, g, mon: (mon[m], 0, g, 0))

    def kernel(*refs):
        tables_kernel(levels, pairs, cut, *refs)

    return pl.pallas_call(
        kernel,
        grid_spec=pltpu.PrefetchScalarGridSpec(
            num_scalar_prefetch=1,
            grid=(order.shape[0], lat_rows // tall),
            in_specs=[
                month_block(),
                month_block(),
                month_block(),
                pl.BlockSpec((levels, tall, lon_cells), lambda m, g, mon: (0, g, 0)),
                pl.BlockSpec((tall, lon_cells), lambda m, g, mon: (g, 0)),
                pl.BlockSpec((tall, lon_cells), lambda m, g, mon: (g, 0)),
                pl.BlockSpec((256, 128), lambda m, g, mon: (0, 0)),
            ],
            out_specs=[
                pl.BlockSpec((1, GROUPS, 2, LOW, 256), lambda m, g, mon: (m, g, 0, 0, 0)),
                pl.BlockSpec((1, GROUPS, 2, padded, 128), lambda m, g, mon: (m, g, 0, 0, 0)),
            ],
            scratch_shapes=[pltpu.VMEM((GROUPS, pairs * 16, 256), BF)],
        ),
        out_shape=[
            jax.ShapeDtypeStruct((order.shape[0], blocks, 2, LOW, 256), F32),
            jax.ShapeDtypeStruct((order.shape[0], blocks, 2, padded, 128), F32),
        ],
        name="tables",
    )(order, north_vel, up_vel, dens_class, thickness, basin_id, width, digits)


def unfold(oc, od, levels):
    blocks = oc.shape[0]
    pairs = (levels + 1) // 2
    c = oc.reshape(blocks, 2, LOW, SLOTS, SUB)[:, :, :, : BASINS * HIGHS]
    c = c.reshape(blocks, 2, LOW, BASINS, HIGHS, SUB).transpose(3, 1, 4, 2, 0, 5)
    c = c.reshape(BASINS, 2, CLASSES, blocks * SUB)
    d = od[:, :, :pairs, : 2 * 32].reshape(blocks, 2, pairs, 2, 4, SUB)[:, :, :, :, :BASINS]
    d = d.transpose(4, 1, 3, 2, 0, 5).reshape(BASINS, 2, 2 * pairs, blocks * SUB)[:, :, :levels]
    return c, d


def with_global(tables):
    return jnp.concatenate([jnp.sum(tables, axis=1, keepdims=True), tables], 1)


def body(north_vel, up_vel, dens_class, thickness, basin_id):
    local_members, months, levels, row_count, lon_cells = north_vel.shape
    lons, lats, mems = lax.axis_size("lon"), lax.axis_size("lat"), lax.axis_size("mem")
    mine = lax.axis_index("lon")
    first_row = lax.axis_index("lat") * row_count
    row_index = first_row + jnp.arange(row_count, dtype=jnp.int32)
    latitude = (-78.0 + 156.0 * (row_index.astype(F32) + 0.5) / (row_count * lats)) * (math.pi / 180.0)
    width = jnp.broadcast_to(jnp.cos(latitude)[:, None], (row_count, lon_cells))
    each = months // lons
    order = jnp.concatenate(
        [((mine + s) % lons) * each + jnp.arange(each, dtype=jnp.int32) for s in range(1, lons + 1)]
    )

    def owned(table):
        total = table[(lons - 1) * each :]
        for s in range(1, lons):
            total = total + lax.ppermute(
                table[(s - 1) * each : s * each], "lon", [(i, (i + s) % lons) for i in range(lons)]
            )
        return total

    class_tabs, depth_tabs = [], []
    for e in range(local_members):
        oc, od = lon_tables(order, north_vel[e], up_vel[e], dens_class[e], thickness, basin_id, width)
        c, d = jax.vmap(lambda a, b: unfold(a, b, levels))(owned(oc), owned(od))
        class_tabs.append(c)
        depth_tabs.append(d)
    class_tab, depth_tab = jnp.stack(class_tabs), jnp.stack(depth_tabs)

    block = (jnp.sum(class_tab[:, :, :, 1], -1), jnp.sum(depth_tab[:, :, :, 1], -1))
    carry = jax.tree.map(jnp.zeros_like, block)
    for s in range(1, lats):
        moved = lax.ppermute(block, "lat", [(i, i + s) for i in range(lats - s)])
        carry = jax.tree.map(jnp.add, carry, moved)

    class_south = jnp.cumsum(jnp.cumsum(class_tab[:, :, :, 1], axis=4) + carry[0][..., None], axis=3)
    class_moc = jnp.stack([jnp.cumsum(class_tab[:, :, :, 0], axis=3), class_south], 3)
    depth_south = jnp.cumsum(depth_tab[:, :, :, 1], axis=4) + carry[1][..., None]
    depth_moc = jnp.stack([jnp.cumsum(depth_tab[:, :, :, 0], axis=3), depth_south], 3)

    members = local_members * mems
    if local_members == 1 and mems == 2:
        both = []
        for moc in (class_moc, depth_moc):
            other = lax.ppermute(moc, "mem", [(0, 1), (1, 0)])
            a, b = with_global(moc[0]), with_global(other[0])
            mean = (a + b) / members
            both.append((mean, jnp.sqrt((jnp.square(a - mean) + jnp.square(b - mean)) / (members - 1))))
        (class_mean, class_spread), (depth_mean, depth_spread) = both
    else:
        mocs = (jax.vmap(with_global)(class_moc), jax.vmap(with_global)(depth_moc))
        total = lax.psum(jax.tree.map(lambda x: jnp.sum(x, 0), mocs), "mem")
        class_mean, depth_mean = total[0] / members, total[1] / members
        dev = lax.psum(
            (
                jnp.sum(jnp.square(mocs[0] - class_mean), 0),
                jnp.sum(jnp.square(mocs[1] - depth_mean), 0),
            ),
            "mem",
        )
        class_spread = jnp.sqrt(dev[0] / (members - 1))
        depth_spread = jnp.sqrt(dev[1] / (members - 1))
    return (depth_mean, depth_spread, class_mean, class_spread)


def solution(mesh):
    in_specs = (
        P("mem", None, None, "lat", "lon"),
        P("mem", None, None, "lat", "lon"),
        P("mem", None, None, "lat", "lon"),
        P(None, "lat", "lon"),
        P("lat", "lon"),
    )
    out_specs = (
        P("lon", None, None, None, "lat"),
        P("lon", None, None, None, "lat"),
        P("lon", None, None, None, "lat"),
        P("lon", None, None, None, "lat"),
    )
    return jax.shard_map(body, mesh=mesh, in_specs=in_specs, out_specs=out_specs, check_vma=False)
```

```python
import functools
import math

import jax
import jax.numpy as jnp
from jax import lax
from jax.experimental import pallas as pl
from jax.experimental.pallas import tpu as pltpu
from jax.sharding import PartitionSpec as P

CLASSES = 80
BASINS = 3
LOW = 8
HIGHS = CLASSES // LOW
SUB = 8
SLOTS = 256 // SUB
UNITS = 2

north_unit = 0.02
up_unit = 0.01

F8 = jnp.float8_e4m3fn
BF = jnp.bfloat16
F32 = jnp.float32


def diagonal(parts, row, lane):
    for bit in (4, 2, 1):
        high = (row & bit) != 0
        same = ((lane & bit) != 0) == high
        merged = []
        for i in range(len(parts) // 2):
            u, v = parts[i], parts[i + len(parts) // 2]
            direct = jnp.where(high, v, u)
            other = jnp.where(high, u, v)
            if bit == 4:
                other = pltpu.roll(other, 4, 0)
            else:
                other = jnp.where(high, pltpu.roll(other, bit, 0), pltpu.roll(other, SUB - bit, 0))
            merged.append(jnp.where(same, direct, other))
        parts = merged
    return parts[0]


def tables_kernel(levels, lat_total, n_ref, u_ref, d_ref, t_ref, b_ref, o_ref, f_s):
    lat_rows = b_ref.shape[0]
    pairs = (levels + 1) // 2
    half = f_s.shape[2] // 16
    first_row = lax.axis_index("lat") * lat_rows

    def body(*accs):
        ca, da = accs[:UNITS], accs[UNITS:]
        row = lax.broadcasted_iota(jnp.int32, (SUB, 256), 0)
        lane = lax.broadcasted_iota(jnp.int32, (SUB, 256), 1)
        digits = (lax.broadcasted_iota(jnp.int32, (256, 128), 0) // SUB).astype(F32).astype(BF)
        for block in range(0, lat_rows // SUB, UNITS):
            offs, cn, cu, masks = [], [], [], []
            rows = [slice((block + q) * SUB, (block + q + 1) * SUB) for q in range(UNITS)]
            for q in range(UNITS):
                b = b_ref[rows[q], :]
                offs.append(jnp.where(b > 0, (b - 1) * HIGHS, 2 * SLOTS))
                masks.append([jnp.where(b == i + 1, 1.0, 0.0) for i in range(BASINS)])
                j = first_row + (block + q) * SUB + lax.broadcasted_iota(jnp.int32, (SUB, 128), 0)
                latitude = (-78.0 + 156.0 * (j.astype(F32) + 0.5) / lat_total) * (math.pi / 180.0)
                width = jnp.cos(latitude)
                cn.append(north_unit * width)
                cu.append(up_unit * width)

            def spot(k):
                return slice(k % half * 16, (k % half + 1) * 16), slice(k // half * 128, (k // half + 1) * 128)

            for k in range(levels, 2 * half):
                for q in range(UNITS):
                    f_s[block // UNITS, q, *spot(k)] = jnp.zeros((16, 128), BF)
            for p in range(pairs):
                lhs = [[] for _ in range(UNITS)]
                rhs = [[] for _ in range(UNITS)]
                for k in (p, p + pairs):
                    if k >= levels:
                        for q in range(UNITS):
                            lhs[q].append(jnp.zeros((2 * LOW * SUB, 128), F32))
                            rhs[q].append(jnp.zeros((256, 128), F8))
                        continue
                    both = slice(block * SUB, (block + UNITS) * SUB)
                    n16 = n_ref[0, k, both, :].astype(F32)
                    u16 = u_ref[0, k, both, :].astype(F32)
                    for q in range(UNITS):
                        part = slice(q * SUB, (q + 1) * SUB)
                        t = t_ref[k, rows[q], :]
                        north = n16[part] * cn[q] * (t.astype(F32) * 0.001)
                        rise = jnp.where(t > 0, u16[part] * cu[q], 0.0)
                        f_s[block // UNITS, q, *spot(k)] = jnp.concatenate([north, rise], 0).astype(BF)
                        d = d_ref[0, k, rows[q], :]
                        high = ((d // LOW if LOW != 8 else d >> 3) + offs[q]).astype(F32)
                        high = jnp.concatenate([high, high], 0).astype(BF)
                        low = d & (LOW - 1)
                        moving = []
                        for x in range(LOW):
                            upto = low <= x
                            moving += [jnp.where(upto, north, 0.0), jnp.where(upto, rise, 0.0)]
                        lhs[q].append(jnp.concatenate(moving, 0))
                        hit = jnp.concatenate([high] * 16, 0) == digits
                        rhs[q].append(jnp.where(hit, F8(1), F8(0)))
                for q in range(UNITS):
                    pltpu.matmul_push_rhs(
                        jnp.concatenate(rhs[q], 1), staging_register=p % 2, mxu_index=q, transpose=True
                    )
                for q in range(UNITS):
                    pltpu.matmul_acc_lhs(ca[q], jnp.concatenate(lhs[q], 1), load_staged_rhs=p % 2)
            zero = jnp.zeros((SUB, 128), F32)
            for c in range(half // SUB):
                staged = (pairs + c) % 2
                for q in range(UNITS):
                    left, right = [zero] * SLOTS, [zero] * SLOTS
                    at = 2 * BASINS * c
                    left[at : at + BASINS] = masks[q]
                    right[at + BASINS : at + 2 * BASINS] = masks[q]
                    held = jnp.concatenate([jnp.concatenate(left, 0), jnp.concatenate(right, 0)], 1)
                    pltpu.matmul_push_rhs(
                        held.astype(F8), staging_register=staged, mxu_index=q, transpose=True
                    )
                for q in range(UNITS):
                    pltpu.matmul_acc_lhs(
                        da[q], f_s[block // UNITS, q, c * 128 : (c + 1) * 128, :], load_staged_rhs=staged
                    )
            for which, acc in enumerate((ca, da)):
                for q in range(UNITS):
                    x = pltpu.matmul_pop(acc[q])
                    for s in range(2):
                        parts = [x[(2 * l + s) * SUB : (2 * l + s + 1) * SUB] for l in range(SUB)]
                        o_ref[0, which, block + q, s] = diagonal(parts, row, lane)

    accs = [pltpu.ACC(q)((2 * LOW * SUB, 256), F32) for _ in range(2) for q in range(UNITS)]
    pl.run_scoped(body, *accs)


def lon_tables(first_month, count, lat_total, lons, each, north_vel, up_vel, dens_class, thickness, basin_id):
    _, levels, lat_rows, lon_cells = north_vel.shape
    half = -(-((levels + 1) // 2) // SUB) * SUB
    months = lons * each

    def month(m):
        return (lax.axis_index("lon") * each + first_month + m) % months

    def month_block():
        return pl.BlockSpec((1, levels, lat_rows, lon_cells), lambda m: (month(m), 0, 0, 0))

    blocks = lat_rows // SUB
    return pl.pallas_call(
        functools.partial(tables_kernel, levels, lat_total),
        grid=(count,),
        in_specs=[
            month_block(),
            month_block(),
            month_block(),
            pl.BlockSpec((levels, lat_rows, lon_cells), lambda m: (0, 0, 0)),
            pl.BlockSpec((lat_rows, lon_cells), lambda m: (0, 0)),
        ],
        out_specs=pl.BlockSpec((1, 2, blocks, 2, SUB, 256), lambda m: (m, 0, 0, 0, 0, 0)),
        out_shape=jax.ShapeDtypeStruct((count, 2, blocks, 2, SUB, 256), F32),
        scratch_shapes=[pltpu.VMEM((blocks // UNITS, UNITS, half * 16, 256), BF)],
        name="tables",
    )(north_vel, up_vel, dens_class, thickness, basin_id)


def summary_kernel(*refs):
    o_ref = refs[-1]
    lane = lax.broadcasted_iota(jnp.int32, (SUB, 128), 1)
    for e, ref in enumerate(refs[:-1]):
        for w in range(2):
            for h in range(2):
                x = [ref[0, w, g, 0, :, h * 128 : (h + 1) * 128] for g in range(ref.shape[2])]
                x = sum(x[1:], x[0])
                for shift in (1, 2, 4):
                    x = x + pltpu.roll(x, 128 - shift, 1)
                o_ref[0, e, w, :, h * 128 : (h + 1) * 128] = jnp.where(lane & (SUB - 1) == 0, x, 0.0)


def carry_summary(tables):
    each, _, blocks = tables[0].shape[:3]
    spec = pl.BlockSpec((1, 2, blocks, 1, SUB, 256), lambda m: (m, 0, 0, 1, 0, 0))
    return pl.pallas_call(
        summary_kernel,
        grid=(each,),
        in_specs=[spec] * len(tables),
        out_specs=pl.BlockSpec((1, len(tables), 2, SUB, 256), lambda m: (m, 0, 0, 0, 0)),
        out_shape=jax.ShapeDtypeStruct((each, len(tables), 2, SUB, 256), F32),
        name="summary",
    )(*tables)


def packed(blocks, row, lane):
    out = []
    for h in range(2):
        u = [b[:, h * 128 : (h + 1) * 128] for b in blocks]
        u = [x if g == 0 else pltpu.roll(x, SUB * g, 1) for g, x in enumerate(u)]
        for r in range(4):
            pick = ((lane >> 3) - r) & 3
            c = jnp.where(pick == 0, u[0], jnp.where(pick == 1, u[1], jnp.where(pick == 2, u[2], u[3])))
            out.append(c if r == 0 else pltpu.roll(c, 128 - SUB * r, 1))
    return out


def finish_kernel(members, levels, stream, carries, *refs):
    tables, refs = refs[:members], refs[members:]
    moved, refs = refs[:carries], refs[carries:]
    outs = refs[-4 if members == 2 else -2 :]
    row = lax.broadcasted_iota(jnp.int32, (SUB, 128), 0)
    lane = lax.broadcasted_iota(jnp.int32, (SUB, 128), 1)
    lat_rows = outs[0].shape[-1]
    kinds = len(outs) // 2
    for w in range(2):
        tiles = []
        for e in range(members):
            blocks = [tables[e][0, w, g, 0] for g in range(4)]
            if carries:
                for s in range(1, carries + 1):
                    south = moved[s - 1][0, e, w]
                    blocks[0] = blocks[0] + jnp.where(lax.axis_index("lat") >= s, south, 0.0)
            part = packed(blocks, row, lane)
            if stream == 1:
                for shift in (1, 2, 4, 8, 16):
                    keep = lane & 31 >= shift
                    part = [x + jnp.where(keep, pltpu.roll(x, shift, 1), 0.0) for x in part]
            elif w == 1:
                for shift in (1, 2, 4):
                    part = [x + jnp.where(row >= shift, pltpu.roll(x, shift, 0), 0.0) for x in part]

            def tile(slot, part=part):
                x = part[slot // 16 * 4 + slot % 4]
                t = slot % 16 // 4
                return x if t == 0 else pltpu.roll(x, 128 - 32 * t, 1)

            tiles.append(tile)
        before = [[None] * BASINS for _ in range(members)]
        count = CLASSES // SUB if w == 0 else -(-levels // SUB)
        for i in range(count):
            moc = []
            for e in range(members):
                regions = []
                for b in range(BASINS):
                    if w == 0:
                        slot = b * HIGHS + i
                    else:
                        slot = i % 5 * 2 * BASINS + i // 5 * BASINS + b
                    x = tiles[e](slot)
                    if w == 0 or stream == 0:
                        total = jnp.broadcast_to(x[SUB - 1 : SUB], x.shape)
                        old = before[e][b]
                        if old is not None:
                            x = x + old
                            total = total + old
                        before[e][b] = total
                    regions.append(x)
                moc.append([regions[0] + regions[1] + regions[2]] + regions)
            size = min(SUB, (CLASSES if w == 0 else levels) - i * SUB)
            for r in range(BASINS + 1):
                if members == 2:
                    a, b = moc[0][r], moc[1][r]
                    values = ((a + b) * 0.5, jnp.abs(a - b) * math.sqrt(0.5))
                else:
                    values = (moc[0][r],)
                for v, ref in zip(values, outs[:kinds] if w == 1 else outs[kinds:]):
                    ref[0, r, 0, i * SUB : i * SUB + size, :] = v[:size, :lat_rows]


def finish(tables, moved, earlier, levels, stream):
    members = len(tables)
    each, _, blocks = tables[0].shape[:3]
    rows = blocks * SUB
    table = pl.BlockSpec((1, 2, blocks, 1, SUB, 256), lambda m: (m, 0, 0, stream, 0, 0))
    carry = pl.BlockSpec((1, members, 2, SUB, 256), lambda m: (m, 0, 0, 0, 0))
    sizes = [levels] * members + [CLASSES] * members

    def out_block(size):
        return pl.BlockSpec((1, BASINS + 1, 1, size, rows), lambda m: (m, 0, stream, 0, 0))

    first = members + len(moved)
    return pl.pallas_call(
        functools.partial(finish_kernel, members, levels, stream, len(moved)),
        grid=(each,),
        in_specs=[table] * members
        + [carry] * len(moved)
        + [pl.BlockSpec(memory_space=pl.ANY)] * len(earlier),
        out_specs=[out_block(size) for size in sizes],
        out_shape=[jax.ShapeDtypeStruct((each, BASINS + 1, 2, size, rows), F32) for size in sizes],
        input_output_aliases={first + i: i for i in range(len(earlier))},
        name="finish_up" if stream else "finish_north",
    )(*tables, *moved, *earlier)


def body(north_vel, up_vel, dens_class, thickness, basin_id):
    local_members, months, levels, row_count, lon_cells = north_vel.shape
    lons, lats, mems = lax.axis_size("lon"), lax.axis_size("lat"), lax.axis_size("mem")
    each = months // lons
    members = local_members * mems

    tables = []
    for e in range(local_members):
        fields = (north_vel[e], up_vel[e], dens_class[e], thickness, basin_id)
        others = lon_tables(each, (lons - 1) * each, row_count * lats, lons, each, *fields)
        arrived = [
            lax.ppermute(others[(s - 1) * each : s * each], "lon", [(i, (i + s) % lons) for i in range(lons)])
            for s in range(1, lons)
        ]
        total = lon_tables(0, each, row_count * lats, lons, each, *fields)
        for part in arrived:
            total = total + part
        tables.append(total)

    def south(summary):
        return [lax.ppermute(summary, "lat", [(i, (i + s) % lats) for i in range(lats)]) for s in range(1, lats)]

    if local_members == 1 and mems == 2:
        pair = [tables[0], lax.ppermute(tables[0], "mem", [(0, 1), (1, 0)])]
        moved = south(carry_summary(pair))
        outs = finish(pair, [], [], levels, 0)
        return tuple(finish(pair, moved, outs, levels, 1))

    mocs = []
    for table in tables:
        moved = south(carry_summary([table]))
        mocs.append(finish([table], moved, finish([table], [], [], levels, 0), levels, 1))
    outs = []
    for i in range(2):
        stack = jnp.stack([moc[i] for moc in mocs])
        mean = lax.psum(jnp.sum(stack, 0), "mem") / members
        dev = lax.psum(jnp.sum(jnp.square(stack - mean), 0), "mem")
        outs += [mean, jnp.sqrt(dev / (members - 1))]
    return tuple(outs)


def solution(mesh):
    in_specs = (
        P("mem", None, None, "lat", "lon"),
        P("mem", None, None, "lat", "lon"),
        P("mem", None, None, "lat", "lon"),
        P(None, "lat", "lon"),
        P("lat", "lon"),
    )
    out_specs = (
        P("lon", None, None, None, "lat"),
        P("lon", None, None, None, "lat"),
        P("lon", None, None, None, "lat"),
        P("lon", None, None, None, "lat"),
    )
    return jax.shard_map(body, mesh=mesh, in_specs=in_specs, out_specs=out_specs, check_vma=False)
```

```python
import functools
import math

import jax
import jax.numpy as jnp
from jax import lax
from jax.experimental import pallas as pl
from jax.experimental.pallas import tpu as pltpu
from jax.sharding import PartitionSpec as P

CLASSES = 80
BASINS = 3
LOW = 8
HIGHS = CLASSES // LOW
SUB = 8
SLOTS = 256 // SUB
UNITS = 2

TABLES_VMEM = 60 << 20
SMALL_VMEM = 8 << 20

north_unit = 0.02
up_unit = 0.01

F8 = jnp.float8_e4m3fn
BF = jnp.bfloat16
F32 = jnp.float32


def diagonal(parts, row, lane):
    for bit in (4, 2, 1):
        high = (lane & bit) != 0
        same = ((row & bit) != 0) == high
        merged = []
        for i in range(len(parts) // 2):
            u, v = parts[i], parts[i + len(parts) // 2]
            direct = jnp.where(high, v, u)
            other = jnp.where(high, u, v)
            other = jnp.where(high, pltpu.roll(other, bit, 1), pltpu.roll(other, 128 - bit, 1))
            merged.append(jnp.where(same, direct, other))
        parts = merged
    return parts[0]


def tables_kernel(levels, lat_total, count, n_ref, u_ref, d_ref, t_ref, b_ref, *refs):
    o_refs, (f_s, *held_out) = refs[:count], refs[count:]
    o_ref = held_out[0] if held_out else o_refs[0]
    lat_rows = b_ref.shape[0]
    pairs = (levels + 1) // 2
    half = f_s.shape[2] // 16
    first_row = lax.axis_index("lat") * lat_rows

    def body(*accs):
        ca, da = accs[:UNITS], accs[UNITS:]
        row = lax.broadcasted_iota(jnp.int32, (SUB, 128), 0)
        lane = lax.broadcasted_iota(jnp.int32, (SUB, 128), 1)
        digits = (lax.broadcasted_iota(jnp.int32, (256, 128), 0) // SUB).astype(F32).astype(BF)
        for block in range(0, lat_rows // SUB, UNITS):
            offs, cn, cu, masks = [], [], [], []
            rows = [slice((block + q) * SUB, (block + q + 1) * SUB) for q in range(UNITS)]
            for q in range(UNITS):
                b = b_ref[rows[q], :]
                offs.append(jnp.where(b > 0, (b - 1) * HIGHS, 2 * SLOTS))
                masks.append([jnp.where(b == i + 1, 1.0, 0.0) for i in range(BASINS)])
                j = first_row + (block + q) * SUB + lax.broadcasted_iota(jnp.int32, (SUB, 128), 0)
                latitude = (-78.0 + 156.0 * (j.astype(F32) + 0.5) / lat_total) * (math.pi / 180.0)
                width = jnp.cos(latitude)
                cn.append(north_unit * width)
                cu.append(up_unit * width)

            def spot(k):
                return slice(k % half * 16, (k % half + 1) * 16), slice(k // half * 128, (k // half + 1) * 128)

            for k in range(levels, 2 * half):
                for q in range(UNITS):
                    f_s[block // UNITS, q, *spot(k)] = jnp.zeros((16, 128), BF)
            for p in range(pairs):
                lhs = [[] for _ in range(UNITS)]
                rhs = [[] for _ in range(UNITS)]
                for k in (p, p + pairs):
                    if k >= levels:
                        for q in range(UNITS):
                            lhs[q].append(jnp.zeros((2 * LOW * SUB, 128), F32))
                            rhs[q].append(jnp.zeros((256, 128), F8))
                        continue
                    both = slice(block * SUB, (block + UNITS) * SUB)
                    n16 = n_ref[0, k, both, :].astype(F32)
                    u16 = u_ref[0, k, both, :].astype(F32)
                    for q in range(UNITS):
                        part = slice(q * SUB, (q + 1) * SUB)
                        t = t_ref[k, rows[q], :]
                        north = n16[part] * cn[q] * (t.astype(F32) * 0.001)
                        rise = jnp.where(t > 0, u16[part] * cu[q], 0.0)
                        f_s[block // UNITS, q, *spot(k)] = jnp.concatenate([north, rise], 0).astype(BF)
                        d = d_ref[0, k, rows[q], :]
                        high = ((d // LOW if LOW != 8 else d >> 3) + offs[q]).astype(F32)
                        high = jnp.concatenate([high, high], 0).astype(BF)
                        low = d & (LOW - 1)
                        moving = []
                        for x in range(LOW):
                            hit = low == x
                            moving += [jnp.where(hit, north, 0.0), jnp.where(hit, rise, 0.0)]
                        lhs[q].append(jnp.concatenate(moving, 0))
                        hit = jnp.concatenate([high] * 16, 0) == digits
                        rhs[q].append(jnp.where(hit, F8(1), F8(0)))
                for q in range(UNITS):
                    pltpu.matmul_push_rhs(
                        jnp.concatenate(rhs[q], 1), staging_register=p % 2, mxu_index=q, transpose=True
                    )
                for q in range(UNITS):
                    pltpu.matmul_acc_lhs(ca[q], jnp.concatenate(lhs[q], 1), load_staged_rhs=p % 2)
            zero = jnp.zeros((SUB, 128), F32)
            for c in range(half // SUB):
                staged = (pairs + c) % 2
                for q in range(UNITS):
                    left, right = [zero] * SLOTS, [zero] * SLOTS
                    for i in range(BASINS):
                        left[i * HIGHS + c] = masks[q][i]
                        right[i * HIGHS + half // SUB + c] = masks[q][i]
                    held = jnp.concatenate([jnp.concatenate(left, 0), jnp.concatenate(right, 0)], 1)
                    pltpu.matmul_push_rhs(
                        held.astype(F8), staging_register=staged, mxu_index=q, transpose=True
                    )
                for q in range(UNITS):
                    pltpu.matmul_acc_lhs(
                        da[q], f_s[block // UNITS, q, c * 128 : (c + 1) * 128, :], load_staged_rhs=staged
                    )
            for which, acc in enumerate((ca, da)):
                for q in range(UNITS):
                    x = pltpu.matmul_pop(acc[q])
                    for s in range(2):
                        for lanes in (slice(0, 128), slice(128, 256)):
                            parts = [x[(2 * l + s) * SUB : (2 * l + s + 1) * SUB, lanes] for l in range(SUB)]
                            o_ref[which, s, rows[q], lanes] = diagonal(parts, row, lane)

    accs = [pltpu.ACC(q)((2 * LOW * SUB, 256), F32) for _ in range(2) for q in range(UNITS)]
    pl.run_scoped(body, *accs)
    if held_out:
        for m in range(count):

            @pl.when(pl.program_id(0) == m)
            def _(m=m):
                o_refs[m][...] = o_ref[...]


def lon_tables(first_month, count, lat_total, lons, each, north_vel, up_vel, dens_class, thickness, basin_id):
    _, levels, lat_rows, lon_cells = north_vel.shape
    half = -(-((levels + 1) // 2) // SUB) * SUB
    months = lons * each
    table = (2, 2, lat_rows, 256)
    vmem = pl.BlockSpec(memory_space=pltpu.VMEM)

    def month(m):
        return (lax.axis_index("lon") * each + first_month + m) % months

    def month_block():
        return pl.BlockSpec((1, levels, lat_rows, lon_cells), lambda m: (month(m), 0, 0, 0))

    blocks = lat_rows // SUB
    return pl.pallas_call(
        functools.partial(tables_kernel, levels, lat_total, count),
        grid=(count,),
        in_specs=[
            month_block(),
            month_block(),
            month_block(),
            pl.BlockSpec((levels, lat_rows, lon_cells), lambda m: (0, 0, 0)),
            pl.BlockSpec((lat_rows, lon_cells), lambda m: (0, 0)),
        ],
        out_specs=[vmem] * count,
        out_shape=[jax.ShapeDtypeStruct(table, F32)] * count,
        scratch_shapes=[pltpu.VMEM((blocks // UNITS, UNITS, half * 16, 256), BF)]
        + [pltpu.VMEM(table, F32)] * (count > 1),
        compiler_params=pltpu.CompilerParams(vmem_limit_bytes=TABLES_VMEM),
        name="tables",
    )(north_vel, up_vel, dens_class, thickness, basin_id)


def summary_kernel(*refs):
    rows = [jnp.sum(ref[w, 1], axis=0, keepdims=True) for ref in refs[:-1] for w in range(2)]
    rows.append(jnp.zeros((SUB - len(rows), 256), F32))
    refs[-1][...] = jnp.concatenate(rows, 0)


def carry_summary(tables):
    vmem = pl.BlockSpec(memory_space=pltpu.VMEM)
    return pl.pallas_call(
        summary_kernel,
        in_specs=[vmem] * len(tables),
        out_specs=vmem,
        out_shape=jax.ShapeDtypeStruct((SUB, 256), F32),
        compiler_params=pltpu.CompilerParams(vmem_limit_bytes=SMALL_VMEM),
        name="summary",
    )(*tables)


def times_binary(x, held):
    total = 0.0
    for _ in range(3):
        part = x.astype(BF)
        x = x - part.astype(F32)
        total = total + jnp.dot(part, held, preferred_element_type=F32)
    return total


def region_sums(prefix):
    row = lax.broadcasted_iota(jnp.int32, (256, 128), 0)
    column = lax.broadcasted_iota(jnp.int32, (256, 128), 1)
    basin = sum(jnp.where(row >= CLASSES * (i + 1), 1, 0) for i in range(BASINS))
    at = row - CLASSES * basin
    hit = ((at <= column) if prefix else (at == column)) & (column < CLASSES) & (basin < BASINS)
    return jnp.concatenate(
        [jnp.where(hit if r == 0 else hit & (basin == r - 1), 1.0, 0.0).astype(BF) for r in range(BASINS + 1)], 1
    )


def finish_kernel(members, levels, stream, carries, *refs):
    tables, refs = refs[:members], refs[members:]
    moved, refs = refs[:carries], refs[carries:]
    outs = refs[-4 if members == 2 else -2 :]
    kinds = len(outs) // 2
    lat_rows = tables[0].shape[2]
    row = lax.broadcasted_iota(jnp.int32, (SUB, 256), 0)
    operands = []
    for w in range(2):
        stack = []
        for e in range(members):
            x = tables[e][w, stream]
            if stream == 1:
                south = jnp.zeros((1, 256), F32)
                for s in range(1, carries + 1):
                    arrived = moved[s - 1][2 * e + w : 2 * e + w + 1, :]
                    south = south + jnp.where(lax.axis_index("lat") >= s, arrived, 0.0)
                for g in range(lat_rows // SUB):
                    y = x[g * SUB : (g + 1) * SUB]
                    for shift in (1, 2, 4):
                        y = y + jnp.where(row >= shift, pltpu.roll(y, shift, 0), 0.0)
                    y = y + south
                    south = y[SUB - 1 : SUB]
                    stack.append(y)
            else:
                stack.append(x)
        operands.append(jnp.concatenate(stack, 0))
    held = region_sums(True)
    if stream == 0:
        both = times_binary(jnp.concatenate(operands, 0), held)
        mocs = [both[: members * lat_rows], both[members * lat_rows :]]
    else:
        mocs = [times_binary(operands[0], held), times_binary(operands[1], region_sums(False))]
    for w in range(2):
        if members == 2:
            a, b = mocs[w][:lat_rows], mocs[w][lat_rows:]
            values = ((a + b) * 0.5, jnp.abs(a - b) * math.sqrt(0.5))
        else:
            values = (mocs[w],)
        size = CLASSES if w == 0 else levels
        for v, ref in zip(values, outs[:kinds] if w == 1 else outs[kinds:]):
            for r in range(BASINS + 1):
                ref[0, r, 0] = v[:, r * 128 : r * 128 + size]


def finish(tables, moved, earlier, levels, stream):
    members = len(tables)
    rows = tables[0].shape[2]
    vmem = pl.BlockSpec(memory_space=pltpu.VMEM)
    sizes = [levels] * members + [CLASSES] * members

    def out_block(size):
        return pl.BlockSpec((1, BASINS + 1, 1, rows, size), lambda m: (0, 0, stream, 0, 0))

    first = members + len(moved)
    return pl.pallas_call(
        functools.partial(finish_kernel, members, levels, stream, len(moved)),
        grid=(1,),
        in_specs=[vmem] * first + [pl.BlockSpec(memory_space=pl.ANY)] * len(earlier),
        out_specs=[out_block(size) for size in sizes],
        out_shape=[jax.ShapeDtypeStruct((1, BASINS + 1, 2, rows, size), F32) for size in sizes],
        input_output_aliases={first + i: i for i in range(len(earlier))},
        compiler_params=pltpu.CompilerParams(vmem_limit_bytes=SMALL_VMEM),
        name="finish_up" if stream else "finish_north",
    )(*tables, *moved, *earlier)


def body(north_vel, up_vel, dens_class, thickness, basin_id):
    local_members, months, levels, row_count, lon_cells = north_vel.shape
    lons, lats, mems = lax.axis_size("lon"), lax.axis_size("lat"), lax.axis_size("mem")
    each = months // lons
    members = local_members * mems

    def south(summary):
        return [lax.ppermute(summary, "lat", [(i, (i + s) % lats) for i in range(lats)]) for s in range(1, lats)]

    def one_month(tables):
        if local_members == 1 and mems == 2:
            pair = [tables[0], lax.ppermute(tables[0], "mem", [(0, 1), (1, 0)])]
            moved = south(carry_summary(pair))
            return finish(pair, moved, finish(pair, [], [], levels, 0), levels, 1)
        mocs = []
        for table in tables:
            moved = south(carry_summary([table]))
            mocs.append(finish([table], moved, finish([table], [], [], levels, 0), levels, 1))
        outs = []
        for i in range(2):
            stack = jnp.stack([moc[i] for moc in mocs])
            mean = lax.psum(jnp.sum(stack, 0), "mem") / members
            dev = lax.psum(jnp.sum(jnp.square(stack - mean), 0), "mem")
            outs += [mean, jnp.sqrt(dev / (members - 1))]
        return outs

    tables = [[] for _ in range(each)]
    for e in range(local_members):
        fields = (north_vel[e], up_vel[e], dens_class[e], thickness, basin_id)
        others = lon_tables(each, (lons - 1) * each, row_count * lats, lons, each, *fields)
        arrived = [
            [
                lax.ppermute(others[(s - 1) * each + m], "lon", [(i, (i + s) % lons) for i in range(lons)])
                for s in range(1, lons)
            ]
            for m in range(each)
        ]
        own = lon_tables(0, each, row_count * lats, lons, each, *fields)
        for m in range(each):
            tables[m].append(sum(arrived[m], own[m]))
    outs = zip(*[one_month(month) for month in tables])
    return tuple(jnp.swapaxes(jnp.concatenate(out, 0), -1, -2) for out in outs)


def solution(mesh):
    in_specs = (
        P("mem", None, None, "lat", "lon"),
        P("mem", None, None, "lat", "lon"),
        P("mem", None, None, "lat", "lon"),
        P(None, "lat", "lon"),
        P("lat", "lon"),
    )
    out_specs = (
        P("lon", None, None, None, "lat"),
        P("lon", None, None, None, "lat"),
        P("lon", None, None, None, "lat"),
        P("lon", None, None, None, "lat"),
    )
    return jax.shard_map(body, mesh=mesh, in_specs=in_specs, out_specs=out_specs, check_vma=False)
```

```python
import functools
import math

import jax
import jax.numpy as jnp
from jax import lax
from jax.experimental import pallas as pl
from jax.experimental.pallas import tpu as pltpu
from jax.sharding import PartitionSpec as P

CLASSES = 80
BASINS = 3
LOW = 8
HIGHS = CLASSES // LOW
SUB = 8
SLOTS = 256 // SUB
UNITS = 2

TABLES_VMEM = 24 << 20
SMALL_VMEM = 8 << 20

north_unit = 0.02
up_unit = 0.01

F8 = jnp.float8_e4m3fn
BF = jnp.bfloat16
F32 = jnp.float32


def diagonal(parts, row, lane):
    for bit in (4, 2, 1):
        high = (lane & bit) != 0
        same = ((row & bit) != 0) == high
        merged = []
        for i in range(len(parts) // 2):
            u, v = parts[i], parts[i + len(parts) // 2]
            direct = jnp.where(high, v, u)
            other = jnp.where(high, u, v)
            other = jnp.where(high, pltpu.roll(other, bit, 1), pltpu.roll(other, 128 - bit, 1))
            merged.append(jnp.where(same, direct, other))
        parts = merged
    return parts[0]


def fetches(levels, lat_rows, months, hbm, vmem, sem):
    pairs = (levels + 1) // 2
    tall = UNITS * SUB
    plan, used = [], 0

    def copy(src, dst):
        nonlocal used
        used += 1
        return pltpu.make_async_copy(src, dst, sem.at[used - 1])

    *hbm, b = hbm
    *vmem, b_s = vmem
    for m, month in enumerate(months):
        for gp in range(lat_rows // tall):
            rows = pl.ds(gp * tall, tall)
            start = m == 0 and gp == 0
            cuts = [0, pairs // 5, pairs // 2, pairs] if start else [0, pairs]
            parts = []
            for first, last in zip(cuts, cuts[1:]):
                copies = [copy(b, b_s)] if used == 0 else []
                spans = [(first, last), (first + pairs, min(last + pairs, levels))] if start else [(0, levels)]
                for k0, k1 in spans:
                    span = pl.ds(k0, k1 - k0)
                    for i, (src, dst) in enumerate(zip(hbm, vmem)):
                        if i < 3:
                            src, dst = src.at[month], dst.at[m]
                        elif m > 0:
                            continue
                        copies.append(copy(src.at[span, rows, :], dst.at[span, rows, :]))
                parts.append((first, copies))
            plan.append(parts)
    return plan


def copy_count(count, blocks):
    pairs = blocks // UNITS
    return 1 + 3 * 2 * 4 + (pairs - 1) * 4 + (count - 1) * pairs * 3


def tables_kernel(levels, lat_total, count, month, rest, *refs):
    fields, refs = refs[:5], refs[5:]
    o_refs, refs = refs[:count], refs[count:]
    lat_rows = fields[4].shape[0]
    plan, kept = [], []
    if month is None:
        (f_s,) = refs
        local = fields
    else:
        keep, refs = refs[: 3 * len(rest)], refs[3 * len(rest) :]
        t_keep, b_keep, f_s, *scratch, sem, keep_sem = refs
        local = [*scratch, t_keep, b_keep]
        plan = fetches(levels, lat_rows, [month(m) for m in range(count)], fields, local, sem)
        for parts in plan:
            for _, copies in parts:
                for c in copies:
                    c.start()
        for i, months in enumerate(rest):
            for f in range(3):
                for m in range(len(months)):
                    at = keep_sem.at[len(kept)]
                    kept.append(pltpu.make_async_copy(fields[f].at[month(months[m])], keep[3 * i + f].at[m], at))
        for c in kept:
            c.start()
    n_ref, u_ref, d_ref, t_ref, b_ref = local
    pairs = (levels + 1) // 2
    half = f_s.shape[2] // 16
    first_row = lax.axis_index("lat") * lat_rows

    def body(*accs):
        ca, da = accs[:UNITS], accs[UNITS:]
        row = lax.broadcasted_iota(jnp.int32, (SUB, 128), 0)
        lane = lax.broadcasted_iota(jnp.int32, (SUB, 128), 1)
        digits = (lax.broadcasted_iota(jnp.int32, (256, 128), 0) // SUB).astype(F32).astype(BF)
        for m, block in [(m, block) for m in range(count) for block in range(0, lat_rows // SUB, UNITS)]:
            unit = m * (lat_rows // SUB // UNITS) + block // UNITS
            waits = dict(plan[0]) if unit == 0 and plan else {}
            if unit + 1 < len(plan):
                waits[pairs - 8] = [c for _, copies in plan[unit + 1] for c in copies]
            elif plan:
                waits[pairs - 8] = kept
            for c in waits.pop(0, []):
                c.wait()
            o_ref = o_refs[m]
            offs, cn, cu, masks = [], [], [], []
            rows = [slice((block + q) * SUB, (block + q + 1) * SUB) for q in range(UNITS)]
            for q in range(UNITS):
                b = b_ref[rows[q], :]
                offs.append(jnp.where(b > 0, (b - 1) * HIGHS, 2 * SLOTS))
                masks.append([jnp.where(b == i + 1, 1.0, 0.0) for i in range(BASINS)])
                j = first_row + (block + q) * SUB + lax.broadcasted_iota(jnp.int32, (SUB, 128), 0)
                latitude = (-78.0 + 156.0 * (j.astype(F32) + 0.5) / lat_total) * (math.pi / 180.0)
                width = jnp.cos(latitude)
                cn.append(north_unit * width)
                cu.append(up_unit * width)

            def spot(k):
                return slice(k % half * 16, (k % half + 1) * 16), slice(k // half * 128, (k // half + 1) * 128)

            for k in range(levels, 2 * half):
                for q in range(UNITS):
                    f_s[block // UNITS, q, *spot(k)] = jnp.zeros((16, 128), BF)
            for p in range(pairs):
                for c in waits.pop(p, []):
                    c.wait()
                lhs = [[] for _ in range(UNITS)]
                rhs = [[] for _ in range(UNITS)]
                for k in (p, p + pairs):
                    if k >= levels:
                        for q in range(UNITS):
                            lhs[q].append(jnp.zeros((2 * LOW * SUB, 128), F32))
                            rhs[q].append(jnp.zeros((256, 128), F8))
                        continue
                    both = slice(block * SUB, (block + UNITS) * SUB)
                    n16 = n_ref[m, k, both, :].astype(F32)
                    u16 = u_ref[m, k, both, :].astype(F32)
                    for q in range(UNITS):
                        part = slice(q * SUB, (q + 1) * SUB)
                        t = t_ref[k, rows[q], :]
                        north = n16[part] * cn[q] * (t.astype(F32) * 0.001)
                        rise = jnp.where(t > 0, u16[part] * cu[q], 0.0)
                        f_s[block // UNITS, q, *spot(k)] = jnp.concatenate([north, rise], 0).astype(BF)
                        d = d_ref[m, k, rows[q], :]
                        high = ((d // LOW if LOW != 8 else d >> 3) + offs[q]).astype(F32)
                        high = jnp.concatenate([high, high], 0).astype(BF)
                        low = d & (LOW - 1)
                        moving = []
                        for x in range(LOW):
                            hit = low == x
                            moving += [jnp.where(hit, north, 0.0), jnp.where(hit, rise, 0.0)]
                        lhs[q].append(jnp.concatenate(moving, 0))
                        hit = jnp.concatenate([high] * 16, 0) == digits
                        rhs[q].append(jnp.where(hit, F8(1), F8(0)))
                for q in range(UNITS):
                    pltpu.matmul_push_rhs(
                        jnp.concatenate(rhs[q], 1), staging_register=p % 2, mxu_index=q, transpose=True
                    )
                for q in range(UNITS):
                    pltpu.matmul_acc_lhs(ca[q], jnp.concatenate(lhs[q], 1), load_staged_rhs=p % 2)
            zero = jnp.zeros((SUB, 128), F32)
            for c in range(half // SUB):
                staged = (pairs + c) % 2
                for q in range(UNITS):
                    left, right = [zero] * SLOTS, [zero] * SLOTS
                    for i in range(BASINS):
                        left[i * HIGHS + c] = masks[q][i]
                        right[i * HIGHS + half // SUB + c] = masks[q][i]
                    held = jnp.concatenate([jnp.concatenate(left, 0), jnp.concatenate(right, 0)], 1)
                    pltpu.matmul_push_rhs(
                        held.astype(F8), staging_register=staged, mxu_index=q, transpose=True
                    )
                for q in range(UNITS):
                    pltpu.matmul_acc_lhs(
                        da[q], f_s[block // UNITS, q, c * 128 : (c + 1) * 128, :], load_staged_rhs=staged
                    )
            for which, acc in enumerate((ca, da)):
                for q in range(UNITS):
                    x = pltpu.matmul_pop(acc[q])
                    for s in range(2):
                        for lanes in (slice(0, 128), slice(128, 256)):
                            parts = [x[(2 * l + s) * SUB : (2 * l + s + 1) * SUB, lanes] for l in range(SUB)]
                            o_ref[which, s, rows[q], lanes] = diagonal(parts, row, lane)

    accs = [pltpu.ACC(q)((2 * LOW * SUB, 256), F32) for _ in range(2) for q in range(UNITS)]
    pl.run_scoped(body, *accs)


def lon_tables(count, lat_total, month, rest, fields):
    levels, lat_rows, lon_cells = fields[3].shape
    half = -(-((levels + 1) // 2) // SUB) * SUB
    blocks = lat_rows // SUB
    vmem = pl.BlockSpec(memory_space=pltpu.VMEM)
    outs = [jax.ShapeDtypeStruct((2, 2, lat_rows, 256), F32)] * count
    scratch = [pltpu.VMEM((blocks // UNITS, UNITS, half * 16, 256), BF)]
    if month is not None:
        fields = [pltpu.with_memory_space_constraint(x, pltpu.HBM) for x in fields]
        outs = outs + [jax.ShapeDtypeStruct((len(ms), *x.shape[1:]), x.dtype) for ms in rest for x in fields[:3]]
        outs = outs + [jax.ShapeDtypeStruct(x.shape, x.dtype) for x in fields[3:]]
        scratch += [pltpu.VMEM((count, *x.shape[1:]), x.dtype) for x in fields[:3]]
        scratch += [
            pltpu.SemaphoreType.DMA((copy_count(count, blocks),)),
            pltpu.SemaphoreType.DMA((3 * sum(len(ms) for ms in rest),)),
        ]
    return pl.pallas_call(
        functools.partial(tables_kernel, levels, lat_total, count, month, rest),
        in_specs=[vmem if month is None else pl.BlockSpec(memory_space=pltpu.HBM)] * 5,
        out_specs=[vmem] * len(outs),
        out_shape=outs,
        scratch_shapes=scratch,
        compiler_params=pltpu.CompilerParams(vmem_limit_bytes=TABLES_VMEM),
        name="tables",
    )(*fields)


def summary_kernel(*refs):
    rows = [jnp.sum(ref[w, 1], axis=0, keepdims=True) for ref in refs[:-1] for w in range(2)]
    rows.append(jnp.zeros((SUB - len(rows), 256), F32))
    refs[-1][...] = jnp.concatenate(rows, 0)


def carry_summary(tables):
    vmem = pl.BlockSpec(memory_space=pltpu.VMEM)
    return pl.pallas_call(
        summary_kernel,
        in_specs=[vmem] * len(tables),
        out_specs=vmem,
        out_shape=jax.ShapeDtypeStruct((SUB, 256), F32),
        compiler_params=pltpu.CompilerParams(vmem_limit_bytes=SMALL_VMEM),
        name="summary",
    )(*tables)


def times_binary(x, held):
    total = 0.0
    for _ in range(3):
        part = x.astype(BF)
        x = x - part.astype(F32)
        total = total + jnp.dot(part, held, preferred_element_type=F32)
    return total


def region_sums(prefix):
    row = lax.broadcasted_iota(jnp.int32, (256, 128), 0)
    column = lax.broadcasted_iota(jnp.int32, (256, 128), 1)
    basin = sum(jnp.where(row >= CLASSES * (i + 1), 1, 0) for i in range(BASINS))
    at = row - CLASSES * basin
    hit = ((at <= column) if prefix else (at == column)) & (column < CLASSES) & (basin < BASINS)
    return jnp.concatenate(
        [jnp.where(hit if r == 0 else hit & (basin == r - 1), 1.0, 0.0).astype(BF) for r in range(BASINS + 1)], 1
    )


def finish_kernel(members, levels, stream, carries, *refs):
    tables, refs = refs[:members], refs[members:]
    moved, refs = refs[:carries], refs[carries:]
    outs = refs[-4 if members == 2 else -2 :]
    kinds = len(outs) // 2
    lat_rows = tables[0].shape[2]
    row = lax.broadcasted_iota(jnp.int32, (SUB, 256), 0)
    operands = []
    for w in range(2):
        stack = []
        for e in range(members):
            x = tables[e][w, stream]
            if stream == 1:
                south = jnp.zeros((1, 256), F32)
                for s in range(1, carries + 1):
                    arrived = moved[s - 1][2 * e + w : 2 * e + w + 1, :]
                    south = south + jnp.where(lax.axis_index("lat") >= s, arrived, 0.0)
                for g in range(lat_rows // SUB):
                    y = x[g * SUB : (g + 1) * SUB]
                    for shift in (1, 2, 4):
                        y = y + jnp.where(row >= shift, pltpu.roll(y, shift, 0), 0.0)
                    y = y + south
                    south = y[SUB - 1 : SUB]
                    stack.append(y)
            else:
                stack.append(x)
        operands.append(jnp.concatenate(stack, 0))
    held = region_sums(True)
    if stream == 0:
        both = times_binary(jnp.concatenate(operands, 0), held)
        mocs = [both[: members * lat_rows], both[members * lat_rows :]]
    else:
        mocs = [times_binary(operands[0], held), times_binary(operands[1], region_sums(False))]
    for w in range(2):
        if members == 2:
            a, b = mocs[w][:lat_rows], mocs[w][lat_rows:]
            values = ((a + b) * 0.5, jnp.abs(a - b) * math.sqrt(0.5))
        else:
            values = (mocs[w],)
        size = CLASSES if w == 0 else levels
        for v, ref in zip(values, outs[:kinds] if w == 1 else outs[kinds:]):
            for r in range(BASINS + 1):
                ref[0, r, 0] = v[:, r * 128 : r * 128 + size]


def finish(tables, moved, earlier, levels, stream):
    members = len(tables)
    rows = tables[0].shape[2]
    vmem = pl.BlockSpec(memory_space=pltpu.VMEM)
    sizes = [levels] * members + [CLASSES] * members

    def out_block(size):
        return pl.BlockSpec((1, BASINS + 1, 1, rows, size), lambda m: (0, 0, stream, 0, 0))

    first = members + len(moved)
    return pl.pallas_call(
        functools.partial(finish_kernel, members, levels, stream, len(moved)),
        grid=(1,),
        in_specs=[vmem] * first + [pl.BlockSpec(memory_space=pl.ANY)] * len(earlier),
        out_specs=[out_block(size) for size in sizes],
        out_shape=[jax.ShapeDtypeStruct((1, BASINS + 1, 2, rows, size), F32) for size in sizes],
        input_output_aliases={first + i: i for i in range(len(earlier))},
        compiler_params=pltpu.CompilerParams(vmem_limit_bytes=SMALL_VMEM),
        name="finish_up" if stream else "finish_north",
    )(*tables, *moved, *earlier)


def body(north_vel, up_vel, dens_class, thickness, basin_id):
    local_members, months, levels, row_count, lon_cells = north_vel.shape
    lons, lats, mems = lax.axis_size("lon"), lax.axis_size("lat"), lax.axis_size("mem")
    each = months // lons
    members = local_members * mems

    def south(summary):
        return [lax.ppermute(summary, "lat", [(i, (i + s) % lats) for i in range(lats)]) for s in range(1, lats)]

    def one_month(tables):
        if local_members == 1 and mems == 2:
            pair = [tables[0], lax.ppermute(tables[0], "mem", [(0, 1), (1, 0)])]
            moved = south(carry_summary(pair))
            return finish(pair, moved, finish(pair, [], [], levels, 0), levels, 1)
        mocs = []
        for table in tables:
            moved = south(carry_summary([table]))
            mocs.append(finish([table], moved, finish([table], [], [], levels, 0), levels, 1))
        outs = []
        for i in range(2):
            stack = jnp.stack([moc[i] for moc in mocs])
            mean = lax.psum(jnp.sum(stack, 0), "mem") / members
            dev = lax.psum(jnp.sum(jnp.square(stack - mean), 0), "mem")
            outs += [mean, jnp.sqrt(dev / (members - 1))]
        return outs

    if lons & (lons - 1) == 0:
        hops = list(range(lons - 1, -1, -1))

        def owner(i, hop):
            return i ^ hop
    else:
        hops = list(range(1, lons + 1))

        def owner(i, hop):
            return (i + hop) % lons

    todo = [(hop, m) for hop in hops for m in range(each)]
    calls = [call for call in (todo[:-each], todo[-each:]) if call]

    def month(item):
        hop, m = item
        if hop == 0 or hop == lons:
            return lax.axis_index("lon") * each + m
        mine = lax.axis_index("lon")
        target = mine ^ hop if lons & (lons - 1) == 0 else lax.rem(mine + hop, lons)
        return target * each + m

    tables = [[] for _ in range(each)]
    for e in range(local_members):
        fields = (north_vel[e], up_vel[e], dens_class[e], thickness, basin_id)
        parts = [[] for _ in range(each)]
        for i, call in enumerate(calls):
            if i == 0:
                at = lambda x: month(call[x] if isinstance(x, int) else x)
                made = lon_tables(len(call), row_count * lats, at, calls[1:], fields)
                kept = made[len(call) :]
            else:
                at = 3 * (i - 1)
                made = lon_tables(len(call), row_count * lats, None, [], (*kept[at : at + 3], *kept[-2:]))
            for (hop, m), table in zip(call, made):
                if hop % lons:
                    table = lax.ppermute(table, "lon", [(j, owner(j, hop)) for j in range(lons)])
                parts[m].append(table)
        for m in range(each):
            tables[m].append(sum(parts[m][1:], parts[m][0]))
    outs = zip(*[one_month(month) for month in tables])
    return tuple(jnp.swapaxes(jnp.concatenate(out, 0), -1, -2) for out in outs)


def solution(mesh):
    in_specs = (
        P("mem", None, None, "lat", "lon"),
        P("mem", None, None, "lat", "lon"),
        P("mem", None, None, "lat", "lon"),
        P(None, "lat", "lon"),
        P("lat", "lon"),
    )
    out_specs = (
        P("lon", None, None, None, "lat"),
        P("lon", None, None, None, "lat"),
        P("lon", None, None, None, "lat"),
        P("lon", None, None, None, "lat"),
    )
    return jax.shard_map(body, mesh=mesh, in_specs=in_specs, out_specs=out_specs, check_vma=False)
```
